256 devices in a mesh: orb: 4 (over y), grid: 64 (over z, x, core).
Axes of the slice: x: 4, y: 4, z: 8, core: 2. Of those that a mesh axis runs over, the one named last changes fastest.
Arguments:
- orbitals: float32 [256, 2048, 128], P('orb', 'grid'), may hold values from -6 to 6
- previous: float32 [256, 2048, 128], P('orb', 'grid'), may hold values from -6 to 6
- potential: float32 [256, 2048, 128], P('orb', 'grid'), may hold values from -3 to 3
- partners: int32 [256, 3], P(('orb', 'grid')), may hold values from 0 to 255, as said below
- offsets: int32 [256, 3, 3], P(('orb', 'grid')), may hold values from -16 to 16, as said below
Outputs:
- advanced: float32 [256, 2048, 128], P('orb', 'grid')
- exchange_force: float32 [256, 2048, 128], P('orb', 'grid')
The draws below stay inside these ranges and needn't reach their ends.
Inputs may be any that keep to these rules, and one draw needn't show every extreme that they name: `partners`: row n names three different orbitals among n + 1 to n + 4, counted modulo 256; so every intersecting pair is listed once, by its first orbital. There are integer box corners of the orbitals with offsets[n, q, :] = corner[partners[n, q]] - corner[n]; both ends of the range occur in every draw.
All inputs are finite; a program needn't handle non-finite values.
Results may differ from the reference program's by a relative error of at most 0.0003.
Values sent between devices are 32-bit elements; how exact they have to be, the bound alone decides.
No kernel may reach another device: no remote copies, remote signals or barrier semaphores. Data moves between devices by JAX's collectives and lax.ppermute only.
A program may use at most 128 MiB of HBM per device.

```python
import math
import jax
import jax.numpy as jnp
from jax import lax

B = 64
SWEEPS = 4
AHEAD = 4
SHIFT = 16
ROWS = 2048
ORBITALS = 256


def pair_layout(key):
    base_key = jax.random.fold_in(key, 7)
    own_index = jnp.arange(ORBITALS, dtype=jnp.int32)[:, None]
    slot_index = jnp.arange(3, dtype=jnp.int32)[None, :]
    dropped = jax.random.randint(jax.random.fold_in(base_key, 1), (ORBITALS, 1), 0, AHEAD)
    distances = slot_index + 1 + (slot_index >= dropped).astype(jnp.int32)
    scores = jax.random.randint(jax.random.fold_in(base_key, 2), (ORBITALS, 3), 0, 4096) * 3 + slot_index
    ordering = jnp.argsort(scores, axis=1)
    distances = jnp.take_along_axis(distances, ordering, axis=1)
    partners = jnp.remainder(own_index + distances, ORBITALS).astype(jnp.int32)
    corners = jax.random.randint(jax.random.fold_in(base_key, 3), (ORBITALS, 3), 0, SHIFT + 1)
    anchor = jax.random.randint(jax.random.fold_in(base_key, 4), (), 0, ORBITALS)
    position = jnp.remainder(own_index[:, 0] - anchor, ORBITALS)
    pattern = jnp.where(position == 0, 0, jnp.where(position <= AHEAD, SHIFT, jnp.where(position <= 2 * AHEAD, 0, corners[:, 0])))
    corners = corners.at[:, 0].set(pattern.astype(jnp.int32))
    offsets = corners[partners] - corners[:, None, :]
    return (partners, offsets.astype(jnp.int32))


def draw_partners(key, part):
    partners, offsets = pair_layout(key)
    return partners


def draw_offsets(key, part):
    partners, offsets = pair_layout(key)
    return offsets


def level_of(own_key, shape, cuts, smallest, high):
    gain, own = 1.0, jax.random.fold_in(own_key, 6)
    for dim, parts in cuts:
        steps = jnp.exp(jax.random.uniform(jax.random.fold_in(own, dim), (parts,), jnp.float32, smallest / len(cuts), high / len(cuts)))
        gain = gain * jnp.repeat(steps, shape[dim] // parts).reshape([-1 if axis == dim else 1 for axis in range(len(shape))])
    return gain


def scatter_about(key, dims, deviation, reach, shards=(), kind=jnp.bfloat16):
    loudness = level_of(key, dims, shards, -0.22, 0.18) if shards else 1.0
    array = jax.random.normal(key, dims, jnp.float32) * deviation * loudness
    return jnp.minimum(jnp.maximum(array, -reach), reach).astype(kind)


def setup_inputs(seed: int = 0) -> dict:
    key_list = jax.random.split(jax.random.key(seed), 6)
    return {
        "orbitals": scatter_about(key_list[0], (ORBITALS, ROWS, 2 * B), 1.0, 6.0, ((0, 4), (1, 64)), jnp.float32),
        "previous": scatter_about(key_list[1], (ORBITALS, ROWS, 2 * B), 1.0, 6.0, ((0, 4), (1, 64)), jnp.float32),
        "potential": jnp.clip(jax.random.uniform(key_list[2], (ORBITALS, ROWS, 2 * B), jnp.float32, -3.0, 3.0) * level_of(key_list[2], (ORBITALS, ROWS, 2 * B), ((0, 4), (1, 64)), -0.4, 0.0), -3.0, 3.0),
        "partners": draw_partners(jax.random.fold_in(key_list[5], 71), 0),
        "offsets": draw_offsets(jax.random.fold_in(key_list[5], 71), 0),
    }


coulomb_factor = 4.0 * math.pi
exact_share = 0.25
verlet_factor = 0.05
lower_edge = 0.5
upper_edge = 16.0


def apply_operator(grid_field):
    leading = grid_field.ndim - 3
    padded = jnp.pad(grid_field, [(0, 0)] * leading + [(2, 2)] * 3)
    extent = grid_field.shape[-1]

    def displaced(axis_number, offset_cells):
        corner = [2, 2, 2]
        corner[axis_number] = 2 + offset_cells
        return padded[..., corner[0]:corner[0] + extent, corner[1]:corner[1] + extent, corner[2]:corner[2] + extent]

    nearest = displaced(0, 1) + displaced(0, -1) + displaced(1, 1) + displaced(1, -1) + displaced(2, 1) + displaced(2, -1)
    farther = displaced(0, 2) + displaced(0, -2) + displaced(1, 2) + displaced(1, -2) + displaced(2, 2) + displaced(2, -2)
    return 7.5 * grid_field - (4.0 / 3.0) * nearest + (1.0 / 12.0) * farther


def sweep_weights():
    centre = 0.5 * (upper_edge + lower_edge)
    radius = 0.5 * (upper_edge - lower_edge)
    ratio_sigma = centre / radius
    previous_rho = 1.0 / ratio_sigma
    weights = []
    for turn_index in range(SWEEPS - 1):
        current_rho = 1.0 / (2.0 * ratio_sigma - previous_rho)
        weights.append((current_rho * previous_rho, 2.0 * current_rho / radius))
        previous_rho = current_rho
    return centre, weights


def solve_potential(density):
    centre, weights = sweep_weights()
    residual = coulomb_factor * density
    direction = residual / centre
    solution = jnp.zeros_like(density)
    for turn_index in range(SWEEPS):
        solution = solution + direction
        residual = residual - apply_operator(direction)
        if turn_index + 1 < SWEEPS:
            keep_weight, residual_weight = weights[turn_index]
            direction = keep_weight * direction + residual_weight * residual
    return solution


def shift_box(one_box, offset, direction_sign):
    extent = one_box.shape[0]
    reach_cells = extent // 4
    padded = jnp.pad(one_box, reach_cells)
    corner = (reach_cells + direction_sign * offset).astype(jnp.int32)
    return lax.dynamic_slice(padded, (corner[0], corner[1], corner[2]), (extent, extent, extent))


def pair_terms(own_box, partner_boxes, pair_offsets):
    def single(partner_box, offset):
        moved_box = shift_box(partner_box, offset, 1)
        potential_box = solve_potential(own_box * moved_box)
        return potential_box * moved_box, shift_box(potential_box * own_box, offset, -1)

    own_terms, partner_terms = jax.vmap(single)(partner_boxes, pair_offsets)
    return jnp.sum(own_terms, axis=0), partner_terms


def reference(orbitals, previous, potential, partners, offsets):
    orbital_boxes = orbitals.reshape(ORBITALS, B, B, B)

    def visit_orbital(force_sum, orbital_index):
        chosen = partners[orbital_index]
        own_term, partner_term = pair_terms(orbital_boxes[orbital_index], orbital_boxes[chosen], offsets[orbital_index])
        force_sum = force_sum.at[orbital_index].add(own_term)
        force_sum = force_sum.at[chosen].add(partner_term)
        return force_sum, None

    force_sum, unused = lax.scan(visit_orbital, jnp.zeros_like(orbital_boxes), jnp.arange(ORBITALS, dtype=jnp.int32))
    exchange_force = (exact_share * force_sum).reshape(orbitals.shape)
    kinetic = (-0.5 * apply_operator(orbital_boxes)).reshape(orbitals.shape)
    acceleration = kinetic + exchange_force
    advanced = 2.0 * orbitals - previous + verlet_factor * (acceleration - potential * orbitals)
    return advanced, exchange_force
```

```python
import functools

import jax
import jax.numpy as jnp
import numpy as np
from jax import lax
from jax.experimental import pallas as pl
from jax.experimental.pallas import tpu as pltpu
from jax.sharding import PartitionSpec as P

B = 64
SWEEPS = 4
AHEAD = 4
HALF = B // 2
LANES = 2 * B
PAD = 8
HIGH = HALF + 2 * PAD
DEEP = B + 4

coulomb_factor = 4.0 * np.pi
exact_share = 0.25
verlet_factor = 0.05
lower_edge = 0.5
upper_edge = 16.0


def sweep_polynomial():
    centre = 0.5 * (upper_edge + lower_edge)
    radius = 0.5 * (upper_edge - lower_edge)
    sigma = centre / radius
    operator = np.polynomial.Polynomial([centre, radius])
    residual = np.polynomial.Polynomial([coulomb_factor])
    direction = residual / centre
    total = np.polynomial.Polynomial([0.0])
    rho = 1.0 / sigma
    for turn in range(SWEEPS):
        total = total + direction
        residual = residual - operator * direction
        if turn + 1 < SWEEPS:
            following = 1.0 / (2.0 * sigma - rho)
            direction = following * rho * direction + (2.0 * following / radius) * residual
            rho = following
    return centre, radius, [float(c) for c in total.coef]


def lane_masks(rows):
    lane = lax.broadcasted_iota(jnp.int32, (rows, LANES), 1)
    cell = lane & (B - 1)
    return {
        "upper": lane >= B,
        "last": cell < B - 1,
        "first": cell > 0,
        "last2": cell < B - 2,
        "first2": cell > 1,
        "cell": cell,
    }


def stencil_plane(ref, a, masks, weights):
    mid = a + 2
    here = ref[mid, PAD : PAD + HALF, :]
    below = ref[mid, PAD - 1 : PAD - 1 + HALF, :]
    above = ref[mid, PAD + 1 : PAD + 1 + HALF, :]

    def turned(by, mask):
        return jnp.where(mask, pltpu.roll(here, by % LANES, 1), 0.0)

    swapped = pltpu.roll(here + jnp.where(masks["upper"], below, above), B, 1)
    near = (
        swapped
        + (ref[mid - 1, PAD : PAD + HALF, :] + ref[mid + 1, PAD : PAD + HALF, :])
        + (turned(-1, masks["last"]) + turned(1, masks["first"]))
    )
    far = (
        (below + above)
        + (ref[mid - 2, PAD : PAD + HALF, :] + ref[mid + 2, PAD : PAD + HALF, :])
        + (turned(-2, masks["last2"]) + turned(2, masks["first2"]))
    )
    return weights[0] * here + weights[1] * near + weights[2] * far


def clear_edges(ref):
    deep = ref.shape[0]
    zero = jnp.zeros((PAD, LANES), jnp.float32)

    def one(a, carry):
        ref[a, :PAD, :] = zero
        ref[a, PAD + HALF :, :] = zero
        return carry

    lax.fori_loop(0, deep, one, 0, unroll=4)
    if deep == DEEP:
        for a in (0, 1, DEEP - 2, DEEP - 1):
            ref[a] = jnp.zeros((HIGH, LANES), jnp.float32)


def inner_rows(ref):
    lead = (ref.shape[0] - B) // 2
    return ref.at[pl.ds(lead, B), pl.ds(PAD, HALF), :]


def kinetic_kernel(boxes, out_ref, box, sem):
    copy = pltpu.make_async_copy(boxes.at[:, 0], inner_rows(box), sem)
    copy.start()
    clear_edges(box)
    copy.wait()
    masks = lane_masks(HALF)
    weights = (-0.5 * 7.5, 0.5 * 4.0 / 3.0, -0.5 / 12.0)

    def one(a, carry):
        out_ref[a] = stencil_plane(box, a, masks, weights)
        return carry

    lax.fori_loop(0, B, one, 0, unroll=2)


def shifted_plane(ref, a, offset, masks):
    lead = (ref.shape[0] - B) // 2
    o0, o1, o2 = offset
    half = lax.shift_right_arithmetic(o1, 1)
    odd = o1 & 1
    source = a + o0
    inside = jnp.logical_and(source >= 0, source < B)
    source = jnp.clip(source, 0, B - 1) + lead
    low = ref[source, pl.ds(PAD + half, HALF), :]
    high = ref[source, pl.ds(PAD + half + odd, HALF), :]
    mixed = jnp.where(masks["upper"] == (odd == 1), low, high)
    turned = pltpu.roll(mixed, (2 * LANES - o2 - B * odd) & (LANES - 1), 1)
    reached = masks["cell"] + o2
    keep = jnp.logical_and(jnp.logical_and(reached >= 0, reached < B), inside)
    return jnp.where(keep, turned, 0.0)


def pairs_kernel(dist, offs, boxes, peers, kept, sent, own, near, rho, work_a, work_b, moved, force, sems, out_sem):
    own_copy = pltpu.make_async_copy(boxes.at[:, 0], own, sems.at[3])
    own_copy.start()
    sources = {1: peers.at[:, 0], 2: boxes.at[:, 1], 3: peers.at[:, 1], 4: boxes.at[:, 2]}

    def fetch(source, q):
        pltpu.make_async_copy(source, inner_rows(near.at[q]), sems.at[q]).start()

    for q in range(3):
        for far, source in sources.items():
            pl.when(dist[q] == far)(functools.partial(fetch, source, q))
    for q in range(3):
        clear_edges(near.at[q])
    for buffer in (rho, work_a, work_b):
        clear_edges(buffer)
    masks = lane_masks(HALF)
    centre, radius, poly = sweep_polynomial()
    poly = [exact_share * c for c in poly]
    step = ((7.5 - centre) / radius, -4.0 / 3.0 / radius, 1.0 / 12.0 / radius)
    first = tuple(poly[3] * s for s in step)
    rows = pl.ds(PAD, HALF)
    absent = 10 - dist[0] - dist[1] - dist[2]

    def blank(a, carry):
        force[absent, a] = jnp.zeros((HALF, LANES), jnp.float32)
        return carry

    lax.fori_loop(0, B, blank, 0, unroll=4)
    own_copy.wait()
    for q in range(3):
        offset = (offs[3 * q], offs[3 * q + 1], offs[3 * q + 2])
        back = tuple(-o for o in offset)
        partner = near.at[q]
        target = dist[q]
        pltpu.make_async_copy(boxes.at[:, 0], inner_rows(partner), sems.at[q]).wait()

        def overlap(a, carry):
            there = shifted_plane(partner, a, offset, masks)
            moved[a] = there
            rho[a + 2, rows, :] = own[a] * there
            return carry

        def sweep_one(a, carry):
            work_a[a + 2, rows, :] = stencil_plane(rho, a, masks, first) + poly[2] * rho[a + 2, rows, :]
            return carry

        def sweep_two(a, carry):
            work_b[a + 2, rows, :] = stencil_plane(work_a, a, masks, step) + poly[1] * rho[a + 2, rows, :]
            return carry

        def sweep_three(a, carry):
            found = stencil_plane(work_b, a, masks, step) + poly[0] * rho[a + 2, rows, :]
            term = found * moved[a]
            force[0, a] = term if q == 0 else force[0, a] + term
            work_a[a + 2, rows, :] = found * own[a]
            return carry

        def give(a, carry):
            force[target, a] = shifted_plane(work_a, a, back, masks)
            return carry

        for body in (overlap, sweep_one, sweep_two, sweep_three, give):
            lax.fori_loop(0, B, body, 0, unroll=2)
    ends = (kept.at[:, 0], sent.at[:, 0], kept.at[:, 1], sent.at[:, 1], kept.at[:, 2])
    copies = [pltpu.make_async_copy(force.at[k], end, out_sem.at[k]) for k, end in enumerate(ends)]
    for copy in copies:
        copy.start()
    for copy in copies:
        copy.wait()


F32 = jnp.float32
ANY = pl.BlockSpec(memory_space=pl.ANY)
SCALARS = pl.BlockSpec(memory_space=pltpu.SMEM)


def kinetic_of(boxes):
    return pl.pallas_call(
        kinetic_kernel,
        out_shape=jax.ShapeDtypeStruct((B, HALF, LANES), F32),
        in_specs=[ANY],
        out_specs=pl.BlockSpec(memory_space=pltpu.VMEM),
        scratch_shapes=[pltpu.VMEM((DEEP, HIGH, LANES), F32), pltpu.SemaphoreType.DMA],
        cost_estimate=pl.CostEstimate(flops=20 * B**3, transcendentals=0, bytes_accessed=8 * B**3),
        name="kinetic",
    )(boxes)


def pair_forces(dist, offs, boxes, peers):
    padded = pltpu.VMEM((DEEP, HIGH, LANES), F32)
    return pl.pallas_call(
        pairs_kernel,
        out_shape=[
            jax.ShapeDtypeStruct((B, 3, HALF, LANES), F32),
            jax.ShapeDtypeStruct((B, 2, HALF, LANES), F32),
        ],
        in_specs=[SCALARS, SCALARS, ANY, ANY],
        out_specs=[ANY, ANY],
        scratch_shapes=[
            pltpu.VMEM((B, HALF, LANES), F32),
            pltpu.VMEM((3, B, HIGH, LANES), F32),
            padded,
            padded,
            padded,
            pltpu.VMEM((B, HALF, LANES), F32),
            pltpu.VMEM((5, B, HALF, LANES), F32),
            pltpu.SemaphoreType.DMA((4,)),
            pltpu.SemaphoreType.DMA((5,)),
        ],
        cost_estimate=pl.CostEstimate(flops=300 * B**3, transcendentals=0, bytes_accessed=40 * B**3),
        name="pairs",
    )(dist, offs, boxes, peers)


def from_behind(array, axis, by):
    count = lax.axis_size(axis)
    return lax.ppermute(array, axis, [(i, (i + by) % count) for i in range(count)])


def core_swap(array):
    count = lax.axis_size("grid")
    return lax.ppermute(array, "grid", [(i, i ^ 1) for i in range(count)])


def local(orbitals, previous, potential, partners, offsets):
    slabs = lax.axis_size("grid")
    total = lax.axis_size("orb") * slabs
    place = lax.axis_index(("orb", "grid"))
    core = place & 1
    dist = jnp.remainder(partners[0] - place, total)
    offs = offsets.reshape(-1)

    upper = from_behind(orbitals[:AHEAD], "orb", -1)
    longer = jnp.concatenate([orbitals, upper], axis=0)
    windows = jnp.stack([longer[:slabs], longer[2 : 2 + slabs], longer[4 : 4 + slabs]], axis=1)
    boxes = lax.all_to_all(windows, "grid", split_axis=0, concat_axis=0, tiled=True)
    offered = lax.dynamic_slice_in_dim(boxes, 1 - core, 2, axis=1)
    peers = core_swap(offered)
    kinetic = lax.all_to_all(kinetic_of(boxes), "grid", split_axis=0, concat_axis=0, tiled=True)

    kept, sent = pair_forces(dist, offs, boxes, peers)
    given = core_swap(sent)
    even = core == 0
    zero = jnp.zeros_like(given[:, 0])
    summed = kept + jnp.stack(
        [
            jnp.where(even, zero, given[:, 0]),
            jnp.where(even, given[:, 0], given[:, 1]),
            jnp.where(even, given[:, 1], zero),
        ],
        axis=1,
    )
    returned = lax.all_to_all(summed, "grid", split_axis=0, concat_axis=0, tiled=True)
    own, two, four = returned[:, 0], returned[:, 1], returned[:, 2]
    spill = four[slabs - 4 :] + jnp.pad(two[slabs - 2 :], ((0, 2), (0, 0), (0, 0)))
    spill = from_behind(spill, "orb", 1)
    exchange_force = own + jnp.concatenate(
        [spill[:2], spill[2:] + two[:2], two[2 : slabs - 2] + four[: slabs - 4]], axis=0
    )
    advanced = (
        2.0 * orbitals
        - previous
        + verlet_factor * (kinetic + exchange_force - potential * orbitals)
    )
    return advanced, exchange_force


def solution(mesh):
    rows = P("orb", "grid", None)
    return jax.shard_map(
        local,
        mesh=mesh,
        in_specs=(rows, rows, rows, P(("orb", "grid"), None), P(("orb", "grid"), None, None)),
        out_specs=(rows, rows),
        check_vma=False,
    )
```

```python
import functools

import jax
import jax.numpy as jnp
import numpy as np
from jax import lax
from jax.experimental import pallas as pl
from jax.experimental.pallas import tpu as pltpu
from jax.sharding import PartitionSpec as P


B = 64
SWEEPS = 4
AHEAD = 4
HALF = B // 2
LANES = 2 * B
PAD = 8
HIGH = HALF + 2 * PAD
DEEP = B + 4
SPAN = 32

coulomb_factor = 4.0 * np.pi
exact_share = 0.25
verlet_factor = 0.05
lower_edge = 0.5
upper_edge = 16.0


def sweep_polynomial():
    centre = 0.5 * (upper_edge + lower_edge)
    radius = 0.5 * (upper_edge - lower_edge)
    sigma = centre / radius
    operator = np.polynomial.Polynomial([centre, radius])
    residual = np.polynomial.Polynomial([coulomb_factor])
    direction = residual / centre
    total = np.polynomial.Polynomial([0.0])
    rho = 1.0 / sigma
    for turn in range(SWEEPS):
        total = total + direction
        residual = residual - operator * direction
        if turn + 1 < SWEEPS:
            following = 1.0 / (2.0 * sigma - rho)
            direction = following * rho * direction + (2.0 * following / radius) * residual
            rho = following
    return centre, radius, [float(c) for c in total.coef]


def lane_mixers():
    along = np.zeros((LANES, LANES), np.float32)
    across = np.zeros((LANES, LANES), np.float32)
    for lane in range(LANES):
        half, cell = divmod(lane, B)
        for by, weight in ((1, -16.0), (-1, -16.0), (2, 1.0), (-2, 1.0)):
            if 0 <= cell + by < B:
                along[half * B + cell + by, lane] = weight
        across[(1 - half) * B + cell, lane] = -16.0
    return jnp.asarray(np.concatenate([along, along, across, across], axis=0), jnp.bfloat16)


def halves(x):
    high = x.astype(jnp.bfloat16)
    return high, (x - high.astype(jnp.float32)).astype(jnp.bfloat16)


def upper_lanes(rows):
    return lax.broadcasted_iota(jnp.int32, (rows, LANES), 1) >= B


def stencil(ref, a, mixers, centre_weight, scale):
    def read(plane, row):
        return ref[pl.ds(a + 2 + plane, SPAN), PAD + row : PAD + row + HALF, :].reshape(SPAN * HALF, LANES)

    here, below, above = read(0, 0), read(0, -1), read(0, 1)
    side = here + jnp.where(upper_lanes(SPAN * HALF), below, above)
    mixed = jnp.dot(
        jnp.concatenate([*halves(here), *halves(side)], axis=1), mixers, preferred_element_type=jnp.float32
    )
    near = read(-1, 0) + read(1, 0)
    far = (read(-2, 0) + read(2, 0)) + (below + above)
    return here, centre_weight * here + scale * (mixed + (far - 16.0 * near))


def over_spans(body):
    def one(i, carry):
        body(i * SPAN)
        return carry

    lax.fori_loop(0, B // SPAN, one, 0)


def clear_edges(ref):
    deep = ref.shape[0]
    zero = jnp.zeros((PAD, LANES), jnp.float32)

    def one(a, carry):
        ref[a, :PAD, :] = zero
        ref[a, PAD + HALF :, :] = zero
        return carry

    lax.fori_loop(0, deep, one, 0, unroll=4)
    if deep == DEEP:
        for a in (0, 1, DEEP - 2, DEEP - 1):
            ref[a] = jnp.zeros((HIGH, LANES), jnp.float32)


def inner_rows(ref):
    lead = (ref.shape[0] - B) // 2
    return ref.at[pl.ds(lead, B), pl.ds(PAD, HALF), :]


def kinetic_kernel(mix, boxes, out, box, result, sem):
    copy = pltpu.make_async_copy(boxes.at[:, 0], inner_rows(box), sem)
    copy.start()
    clear_edges(box)
    copy.wait()
    mixers = mix[...]

    def body(a):
        _, found = stencil(box, a, mixers, -0.5 * 7.5, -0.5 / 12.0)
        result[pl.ds(a, SPAN)] = found.reshape(SPAN, HALF, LANES)

    over_spans(body)
    back = pltpu.make_async_copy(result, out, sem)
    back.start()
    back.wait()


def shifted_plane(ref, a, offset, upper, cell):
    lead = (ref.shape[0] - B) // 2
    o0, o1, o2 = offset
    half = lax.shift_right_arithmetic(o1, 1)
    odd = o1 & 1
    source = a + o0
    inside = jnp.logical_and(source >= 0, source < B)
    source = jnp.clip(source, 0, B - 1) + lead
    low = ref[source, pl.ds(PAD + half, HALF), :]
    high = ref[source, pl.ds(PAD + half + odd, HALF), :]
    mixed = jnp.where(upper == (odd == 1), low, high)
    turned = pltpu.roll(mixed, (2 * LANES - o2 - B * odd) & (LANES - 1), 1)
    reached = cell + o2
    keep = jnp.logical_and(jnp.logical_and(reached >= 0, reached < B), inside)
    return jnp.where(keep, turned, 0.0)


def pairs_kernel(dist, offs, mix, boxes, peers, order, kept, sent,
                 own, near, rho, work_a, work_b, moved, force, sems, out_sem):
    own_copy = pltpu.make_async_copy(boxes.at[:, 0], own, sems.at[3])
    own_copy.start()
    sources = {1: peers.at[:, 0], 2: boxes.at[:, 1], 3: peers.at[:, 1], 4: boxes.at[:, 2]}
    ends = {0: kept.at[:, 0], 1: sent.at[:, 0], 2: kept.at[:, 1], 3: sent.at[:, 1], 4: kept.at[:, 2]}

    def fetch(source, q):
        pltpu.make_async_copy(source, inner_rows(near.at[q]), sems.at[q]).start()

    def deliver(which, sem):
        pltpu.make_async_copy(force.at[which], ends[which], sem).start()

    for q in range(3):
        for far, source in sources.items():
            pl.when(dist[q] == far)(functools.partial(fetch, source, q))
    absent = 10 - dist[0] - dist[1] - dist[2]

    def blank(a, carry):
        force[absent, a] = jnp.zeros((HALF, LANES), jnp.float32)
        force[0, a] = jnp.zeros((HALF, LANES), jnp.float32)
        return carry

    lax.fori_loop(0, B, blank, 0, unroll=4)
    for which in sources:
        pl.when(absent == which)(functools.partial(deliver, which, out_sem.at[3]))
    for q in range(3):
        clear_edges(near.at[q])
    for buffer in (rho, work_a, work_b):
        clear_edges(buffer)
    cell = lax.broadcasted_iota(jnp.int32, (HALF, LANES), 1) & (B - 1)
    upper = upper_lanes(HALF)
    mixers = mix[...]
    centre, radius, poly = sweep_polynomial()
    poly = [exact_share * c for c in poly]
    centre_weight = (7.5 - centre) / radius
    scale = 1.0 / 12.0 / radius
    rows = pl.ds(PAD, HALF)
    own_copy.wait()

    def pair(q, carry):
        offset = (offs[3 * q], offs[3 * q + 1], offs[3 * q + 2])
        back = tuple(-o for o in offset)
        partner = near.at[q]
        target = dist[q]
        pltpu.make_async_copy(boxes.at[:, 0], inner_rows(partner), sems.at[q]).wait()

        def overlap(a, carry):
            there = shifted_plane(partner, a, offset, upper, cell)
            moved[a] = there
            rho[a + 2, rows, :] = own[a] * there
            return carry

        def sweep_one(a):
            here, found = stencil(rho, a, mixers, poly[3] * centre_weight, poly[3] * scale)
            work_a[pl.ds(a + 2, SPAN), rows, :] = (found + poly[2] * here).reshape(SPAN, HALF, LANES)

        def sweep_two(a):
            _, found = stencil(work_a, a, mixers, centre_weight, scale)
            found = found.reshape(SPAN, HALF, LANES)
            work_b[pl.ds(a + 2, SPAN), rows, :] = found + poly[1] * rho[pl.ds(a + 2, SPAN), rows, :]

        def sweep_three(a):
            _, found = stencil(work_b, a, mixers, centre_weight, scale)
            here = pl.ds(a, SPAN)
            inner = pl.ds(a + 2, SPAN)
            found = found.reshape(SPAN, HALF, LANES) + poly[0] * rho[inner, rows, :]
            force[0, here] += found * moved[here]
            work_a[inner, rows, :] = found * own[here]

        def give(a, carry):
            force[target, a] = shifted_plane(work_a, a, back, upper, cell)
            return carry

        lax.fori_loop(0, B, overlap, 0, unroll=16)
        over_spans(sweep_one)
        over_spans(sweep_two)
        over_spans(sweep_three)
        lax.fori_loop(0, B, give, 0, unroll=16)
        for which in sources:
            pl.when(target == which)(functools.partial(deliver, which, out_sem.at[q]))
        return carry

    lax.fori_loop(0, 3, pair, 0)
    deliver(0, out_sem.at[4])
    for k in range(5):
        pltpu.make_async_copy(force.at[0], ends[0], out_sem.at[k]).wait()


F32 = jnp.float32
ANY = pl.BlockSpec(memory_space=pl.ANY)
WHOLE = pl.BlockSpec(memory_space=pltpu.VMEM)
SCALARS = pl.BlockSpec(memory_space=pltpu.SMEM)


def kinetic_of(boxes):
    return pl.pallas_call(
        kinetic_kernel,
        out_shape=jax.ShapeDtypeStruct((B, HALF, LANES), F32),
        in_specs=[WHOLE, ANY],
        out_specs=ANY,
        scratch_shapes=[
            pltpu.VMEM((DEEP, HIGH, LANES), F32),
            pltpu.VMEM((B, HALF, LANES), F32),
            pltpu.SemaphoreType.DMA,
        ],
        cost_estimate=pl.CostEstimate(flops=20 * B**3, transcendentals=0, bytes_accessed=8 * B**3),
        name="kinetic",
    )(lane_mixers(), boxes)


def pair_forces(dist, offs, boxes, peers, order):
    padded = pltpu.VMEM((DEEP, HIGH, LANES), F32)
    return pl.pallas_call(
        pairs_kernel,
        out_shape=[
            jax.ShapeDtypeStruct((B, 3, HALF, LANES), F32),
            jax.ShapeDtypeStruct((B, 2, HALF, LANES), F32),
        ],
        in_specs=[SCALARS, SCALARS, WHOLE, ANY, ANY, ANY],
        out_specs=[ANY, ANY],
        scratch_shapes=[
            pltpu.VMEM((B, HALF, LANES), F32),
            pltpu.VMEM((3, B, HIGH, LANES), F32),
            padded,
            padded,
            padded,
            pltpu.VMEM((B, HALF, LANES), F32),
            pltpu.VMEM((5, B, HALF, LANES), F32),
            pltpu.SemaphoreType.DMA((4,)),
            pltpu.SemaphoreType.DMA((5,)),
        ],
        cost_estimate=pl.CostEstimate(flops=300 * B**3, transcendentals=0, bytes_accessed=40 * B**3),
        name="pairs",
    )(dist, offs, lane_mixers(), boxes, peers, order)


def from_behind(array, axis, by):
    count = lax.axis_size(axis)
    return lax.ppermute(array, axis, [(i, (i + by) % count) for i in range(count)])


def core_swap(array):
    count = lax.axis_size("grid")
    return lax.ppermute(array, "grid", [(i, i ^ 1) for i in range(count)])


def local(orbitals, previous, potential, partners, offsets):
    slabs = lax.axis_size("grid")
    total = lax.axis_size("orb") * slabs
    place = lax.axis_index(("orb", "grid"))
    core = place & 1
    dist = jnp.remainder(partners[0] - place, total)
    offs = offsets.reshape(-1)

    upper = from_behind(orbitals[:AHEAD], "orb", -1)
    longer = jnp.concatenate([orbitals, upper], axis=0)
    windows = jnp.stack([longer[:slabs], longer[2 : 2 + slabs], longer[4 : 4 + slabs]], axis=1)
    boxes = lax.all_to_all(windows, "grid", split_axis=0, concat_axis=0, tiled=True)
    offered = lax.dynamic_slice_in_dim(boxes, 1 - core, 2, axis=1)
    peers = core_swap(offered)
    own_kinetic = kinetic_of(boxes)
    kinetic = lax.all_to_all(own_kinetic, "grid", split_axis=0, concat_axis=0, tiled=True)
    kept, sent = pair_forces(dist, offs, boxes, peers, own_kinetic)
    given = core_swap(sent)
    even = core == 0
    zero = jnp.zeros_like(given[:, 0])
    summed = kept + jnp.stack(
        [
            jnp.where(even, zero, given[:, 0]),
            jnp.where(even, given[:, 0], given[:, 1]),
            jnp.where(even, given[:, 1], zero),
        ],
        axis=1,
    )
    summed, kinetic = lax.optimization_barrier((summed, kinetic))
    returned = lax.all_to_all(summed, "grid", split_axis=0, concat_axis=0, tiled=True)
    own, two, four = returned[:, 0], returned[:, 1], returned[:, 2]
    spill = four[slabs - 4 :] + jnp.pad(two[slabs - 2 :], ((0, 2), (0, 0), (0, 0)))
    spill = from_behind(spill, "orb", 1)
    exchange_force = own + jnp.concatenate(
        [spill[:2], spill[2:] + two[:2], two[2 : slabs - 2] + four[: slabs - 4]], axis=0
    )
    advanced = (
        2.0 * orbitals
        - previous
        + verlet_factor * (kinetic + exchange_force - potential * orbitals)
    )
    return advanced, exchange_force


def solution(mesh):
    rows = P("orb", "grid", None)
    return jax.shard_map(
        local,
        mesh=mesh,
        in_specs=(rows, rows, rows, P(("orb", "grid"), None), P(("orb", "grid"), None, None)),
        out_specs=(rows, rows),
        check_vma=False,
    )
```

```python
import functools

import jax
import jax.numpy as jnp
import numpy as np
from jax import lax
from jax.experimental import pallas as pl
from jax.experimental.pallas import tpu as pltpu
from jax.sharding import PartitionSpec as P


B = 64
SWEEPS = 4
AHEAD = 4
HALF = B // 2
LANES = 2 * B
PAD = 8
HIGH = HALF + 2 * PAD
DEEP = B + 4
SPAN = 32
GROUP = 8

coulomb_factor = 4.0 * np.pi
exact_share = 0.25
verlet_factor = 0.05
lower_edge = 0.5
upper_edge = 16.0


def sweep_polynomial():
    centre = 0.5 * (upper_edge + lower_edge)
    radius = 0.5 * (upper_edge - lower_edge)
    sigma = centre / radius
    operator = np.polynomial.Polynomial([centre, radius])
    residual = np.polynomial.Polynomial([coulomb_factor])
    direction = residual / centre
    total = np.polynomial.Polynomial([0.0])
    rho = 1.0 / sigma
    for turn in range(SWEEPS):
        total = total + direction
        residual = residual - operator * direction
        if turn + 1 < SWEEPS:
            following = 1.0 / (2.0 * sigma - rho)
            direction = following * rho * direction + (2.0 * following / radius) * residual
            rho = following
    return centre, radius, [float(c) for c in total.coef]


def lane_mixers():
    along = np.zeros((LANES, LANES), np.float32)
    across = np.zeros((LANES, LANES), np.float32)
    for lane in range(LANES):
        half, cell = divmod(lane, B)
        for by, weight in ((1, -16.0), (-1, -16.0), (2, 1.0), (-2, 1.0)):
            if 0 <= cell + by < B:
                along[half * B + cell + by, lane] = weight
        across[(1 - half) * B + cell, lane] = -16.0
    return jnp.asarray(np.concatenate([along, along, across, across], axis=0), jnp.bfloat16)


def halves(x):
    high = x.astype(jnp.bfloat16)
    return high, (x - high.astype(jnp.float32)).astype(jnp.bfloat16)


def upper_lanes(rows):
    return lax.broadcasted_iota(jnp.int32, (rows, LANES), 1) >= B


def stencil(ref, a, mixers, centre_weight, scale):
    def read(plane, row):
        return ref[pl.ds(a + 2 + plane, SPAN), PAD + row : PAD + row + HALF, :].reshape(SPAN * HALF, LANES)

    here, below, above = read(0, 0), read(0, -1), read(0, 1)
    side = here + jnp.where(upper_lanes(SPAN * HALF), below, above)
    mixed = jnp.dot(
        jnp.concatenate([*halves(here), *halves(side)], axis=1), mixers, preferred_element_type=jnp.float32
    )
    near = read(-1, 0) + read(1, 0)
    far = (read(-2, 0) + read(2, 0)) + (below + above)
    return here, centre_weight * here + scale * (mixed + (far - 16.0 * near))


def over_spans(body):
    def one(i, carry):
        body(i * SPAN)
        return carry

    lax.fori_loop(0, B // SPAN, one, 0)


def clear_edges(ref):
    deep = ref.shape[0]
    zero = jnp.zeros((PAD, LANES), jnp.float32)

    def one(a, carry):
        ref[a, :PAD, :] = zero
        ref[a, PAD + HALF :, :] = zero
        return carry

    lax.fori_loop(0, deep, one, 0, unroll=4)
    if deep == DEEP:
        for a in (0, 1, DEEP - 2, DEEP - 1):
            ref[a] = jnp.zeros((HIGH, LANES), jnp.float32)


def inner_rows(ref):
    lead = (ref.shape[0] - B) // 2
    return ref.at[pl.ds(lead, B), pl.ds(PAD, HALF), :]


def slab_kernel(place, mix, own, low, high, peer, peer_low, peer_high, previous, potential, out, box):
    slab = place[0]
    core = slab & 1
    rows = pl.ds(PAD, HALF)

    @pl.when(pl.program_id(0) == 0)
    def _():
        clear_edges(box)

    here = own[...]
    box[:, rows, :] = here
    zero = jnp.zeros_like(here)
    below = jnp.where(slab > 1, low[...], zero)
    above = jnp.where(slab < place[1] - 2, high[...], zero)
    edge = jnp.where(core == 0, peer_low[...], peer_high[...])
    held = jnp.logical_or(jnp.logical_and(core == 0, slab > 1), jnp.logical_and(core == 1, slab < place[1] - 2))
    near = peer[...] + jnp.where(held, edge, zero)
    far = below + above
    flat = here.reshape(GROUP * HALF, LANES)
    lower = box[:, PAD - 1 : PAD - 1 + HALF, :].reshape(GROUP * HALF, LANES)
    upper = box[:, PAD + 1 : PAD + 1 + HALF, :].reshape(GROUP * HALF, LANES)
    side = flat + jnp.where(upper_lanes(GROUP * HALF), lower, upper)
    mixed = jnp.dot(
        jnp.concatenate([*halves(flat), *halves(side)], axis=1), mix[...], preferred_element_type=jnp.float32
    )
    mixed = (mixed + (lower + upper)).reshape(GROUP, HALF, LANES)
    kinetic = -3.75 * here - (mixed + (far - 16.0 * near)) / 24.0
    out[...] = 2.0 * here - previous[...] + verlet_factor * (kinetic - potential[...] * here)


def shifted_plane(ref, a, offset, upper, cell):
    lead = (ref.shape[0] - B) // 2
    o0, o1, o2 = offset
    half = lax.shift_right_arithmetic(o1, 1)
    odd = o1 & 1
    source = a + o0
    inside = jnp.logical_and(source >= 0, source < B)
    source = jnp.clip(source, 0, B - 1) + lead
    low = ref[source, pl.ds(PAD + half, HALF), :]
    high = ref[source, pl.ds(PAD + half + odd, HALF), :]
    mixed = jnp.where(upper == (odd == 1), low, high)
    turned = pltpu.roll(mixed, (2 * LANES - o2 - B * odd) & (LANES - 1), 1)
    reached = cell + o2
    keep = jnp.logical_and(jnp.logical_and(reached >= 0, reached < B), inside)
    return jnp.where(keep, turned, 0.0)


def pairs_kernel(place, partners, offsets, mix, boxes, peers, kept, sent,
                 own, near, rho, work_a, work_b, moved, force, sems, out_sem):
    core = place[0] & 1
    dist = [jnp.remainder(partners[0, q] - place[0] + place[1], place[1]) for q in range(3)]
    own_copy = pltpu.make_async_copy(boxes.at[:, 0], own, sems.at[3])
    own_copy.start()
    sources = {1: peers.at[:, core], 2: boxes.at[:, 1], 3: peers.at[:, 1 + core], 4: boxes.at[:, 2]}
    ends = {0: kept.at[:, 0], 1: sent.at[:, 0], 2: kept.at[:, 1], 3: sent.at[:, 1], 4: kept.at[:, 2]}

    def fetch(source, q):
        pltpu.make_async_copy(source, inner_rows(near.at[q]), sems.at[q]).start()

    def deliver(which, sem):
        pltpu.make_async_copy(force.at[which], ends[which], sem).start()

    for q in range(3):
        for far, source in sources.items():
            pl.when(dist[q] == far)(functools.partial(fetch, source, q))
    absent = 10 - dist[0] - dist[1] - dist[2]

    def blank(a, carry):
        force[absent, a] = jnp.zeros((HALF, LANES), jnp.float32)
        force[0, a] = jnp.zeros((HALF, LANES), jnp.float32)
        return carry

    lax.fori_loop(0, B, blank, 0, unroll=4)
    for which in sources:
        pl.when(absent == which)(functools.partial(deliver, which, out_sem.at[3]))
    for q in range(3):
        clear_edges(near.at[q])
    for buffer in (rho, work_a, work_b):
        clear_edges(buffer)
    cell = lax.broadcasted_iota(jnp.int32, (HALF, LANES), 1) & (B - 1)
    upper = upper_lanes(HALF)
    mixers = mix[...]
    centre, radius, poly = sweep_polynomial()
    poly = [exact_share * c for c in poly]
    centre_weight = (7.5 - centre) / radius
    scale = 1.0 / 12.0 / radius
    rows = pl.ds(PAD, HALF)
    own_copy.wait()

    def pair(q, carry):
        offset = (offsets[0, q, 0], offsets[0, q, 1], offsets[0, q, 2])
        back = tuple(-o for o in offset)
        partner = near.at[q]
        target = jnp.where(q == 0, dist[0], jnp.where(q == 1, dist[1], dist[2]))
        pltpu.make_async_copy(boxes.at[:, 0], inner_rows(partner), sems.at[q]).wait()

        def overlap(a, carry):
            there = shifted_plane(partner, a, offset, upper, cell)
            moved[a] = there
            rho[a + 2, rows, :] = own[a] * there
            return carry

        def sweep_one(a):
            here, found = stencil(rho, a, mixers, poly[3] * centre_weight, poly[3] * scale)
            work_a[pl.ds(a + 2, SPAN), rows, :] = (found + poly[2] * here).reshape(SPAN, HALF, LANES)

        def sweep_two(a):
            _, found = stencil(work_a, a, mixers, centre_weight, scale)
            found = found.reshape(SPAN, HALF, LANES)
            work_b[pl.ds(a + 2, SPAN), rows, :] = found + poly[1] * rho[pl.ds(a + 2, SPAN), rows, :]

        def sweep_three(a):
            _, found = stencil(work_b, a, mixers, centre_weight, scale)
            here = pl.ds(a, SPAN)
            inner = pl.ds(a + 2, SPAN)
            found = found.reshape(SPAN, HALF, LANES) + poly[0] * rho[inner, rows, :]
            force[0, here] += found * moved[here]
            work_a[inner, rows, :] = found * own[here]

        def give(a, carry):
            force[target, a] = shifted_plane(work_a, a, back, upper, cell)
            return carry

        lax.fori_loop(0, B, overlap, 0, unroll=16)
        over_spans(sweep_one)
        over_spans(sweep_two)
        over_spans(sweep_three)
        lax.fori_loop(0, B, give, 0, unroll=16)
        for which in sources:
            pl.when(target == which)(functools.partial(deliver, which, out_sem.at[q]))
        return carry

    lax.fori_loop(0, 3, pair, 0)
    deliver(0, out_sem.at[4])
    for k in range(5):
        pltpu.make_async_copy(force.at[0], ends[0], out_sem.at[k]).wait()


F32 = jnp.float32
ANY = pl.BlockSpec(memory_space=pl.ANY)
WHOLE = pl.BlockSpec(memory_space=pltpu.VMEM)
SCALARS = pl.BlockSpec(memory_space=pltpu.SMEM)


def slab_terms(place, arrays):
    block = pl.BlockSpec((GROUP, HALF, LANES), lambda i: (i, 0, 0))
    return pl.pallas_call(
        slab_kernel,
        grid=(arrays[0].shape[0] // GROUP,),
        out_shape=jax.ShapeDtypeStruct(arrays[0].shape, F32),
        in_specs=[SCALARS, WHOLE] + [block] * len(arrays),
        out_specs=block,
        scratch_shapes=[pltpu.VMEM((GROUP, HIGH, LANES), F32)],
        cost_estimate=pl.CostEstimate(flops=20 * B**3, transcendentals=0, bytes_accessed=36 * B**3),
        name="slab",
    )(place, lane_mixers(), *arrays)


def pair_forces(place, partners, offsets, boxes, peers):
    padded = pltpu.VMEM((DEEP, HIGH, LANES), F32)
    return pl.pallas_call(
        pairs_kernel,
        out_shape=[
            jax.ShapeDtypeStruct((B, 3, HALF, LANES), F32),
            jax.ShapeDtypeStruct((B, 2, HALF, LANES), F32),
        ],
        in_specs=[SCALARS, SCALARS, SCALARS, WHOLE, ANY, ANY],
        out_specs=[ANY, ANY],
        scratch_shapes=[
            pltpu.VMEM((B, HALF, LANES), F32),
            pltpu.VMEM((3, B, HIGH, LANES), F32),
            padded,
            padded,
            padded,
            pltpu.VMEM((B, HALF, LANES), F32),
            pltpu.VMEM((5, B, HALF, LANES), F32),
            pltpu.SemaphoreType.DMA((4,)),
            pltpu.SemaphoreType.DMA((5,)),
        ],
        cost_estimate=pl.CostEstimate(flops=300 * B**3, transcendentals=0, bytes_accessed=40 * B**3),
        name="pairs",
    )(place, partners, offsets, lane_mixers(), boxes, peers)


def from_behind(array, axis, by):
    count = lax.axis_size(axis)
    return lax.ppermute(array, axis, [(i, (i + by) % count) for i in range(count)])


def core_swap(array):
    count = lax.axis_size("grid")
    return lax.ppermute(array, "grid", [(i, i ^ 1) for i in range(count)])


def local(orbitals, previous, potential, partners, offsets):
    slabs = lax.axis_size("grid")
    total = lax.axis_size("orb") * slabs
    index = lax.axis_index("grid")
    even = (index & 1) == 0
    place = jnp.stack([lax.axis_index(("orb", "grid")), jnp.int32(total)])
    slab = jnp.stack([index, jnp.int32(slabs)])

    upper = from_behind(orbitals[:AHEAD], "orb", -1)
    longer = jnp.concatenate([orbitals, upper], axis=0)
    windows = jnp.stack([longer[:slabs], longer[2 : 2 + slabs], longer[4 : 4 + slabs]], axis=1)
    boxes = lax.all_to_all(windows, "grid", split_axis=0, concat_axis=0, tiled=True)
    peers = core_swap(boxes)
    source, _ = lax.optimization_barrier((orbitals, boxes))
    low = from_behind(source, "grid", 2)
    high = from_behind(source, "grid", -2)
    kept, sent = pair_forces(place, partners, offsets, boxes, peers)
    given = core_swap(sent)
    zero = jnp.zeros_like(given[:, 0])
    summed = kept + jnp.stack(
        [
            jnp.where(even, zero, given[:, 0]),
            jnp.where(even, given[:, 0], given[:, 1]),
            jnp.where(even, given[:, 1], zero),
        ],
        axis=1,
    )
    summed, low, high = lax.optimization_barrier((summed, low, high))
    returned = lax.all_to_all(summed, "grid", split_axis=0, concat_axis=0, tiled=True)
    sides = [core_swap(array) for array in (source, low, high)]
    base = slab_terms(slab, [orbitals, low, high, *sides, previous, potential])
    own, two, four = returned[:, 0], returned[:, 1], returned[:, 2]
    spill = four[slabs - 4 :] + jnp.pad(two[slabs - 2 :], ((0, 2), (0, 0), (0, 0)))
    spill = from_behind(spill, "orb", 1)
    exchange_force = own + jnp.concatenate(
        [spill[:2], spill[2:] + two[:2], two[2 : slabs - 2] + four[: slabs - 4]], axis=0
    )
    return base + verlet_factor * exchange_force, exchange_force


def solution(mesh):
    rows = P("orb", "grid", None)
    return jax.shard_map(
        local,
        mesh=mesh,
        in_specs=(rows, rows, rows, P(("orb", "grid"), None), P(("orb", "grid"), None, None)),
        out_specs=(rows, rows),
        check_vma=False,
    )
```

```python
import functools

import jax
import jax.numpy as jnp
import numpy as np
from jax import lax
from jax.experimental import pallas as pl
from jax.experimental.pallas import tpu as pltpu
from jax.sharding import PartitionSpec as P


B = 64
SWEEPS = 4
AHEAD = 4
HALF = B // 2
LANES = 2 * B
PAD = 8
HIGH = HALF + 2 * PAD
DEEP = B + 4
SPAN = 64
GROUP = 8

coulomb_factor = 4.0 * np.pi
exact_share = 0.25
verlet_factor = 0.05
lower_edge = 0.5
upper_edge = 16.0


def sweep_polynomial():
    centre = 0.5 * (upper_edge + lower_edge)
    radius = 0.5 * (upper_edge - lower_edge)
    sigma = centre / radius
    operator = np.polynomial.Polynomial([centre, radius])
    residual = np.polynomial.Polynomial([coulomb_factor])
    direction = residual / centre
    total = np.polynomial.Polynomial([0.0])
    rho = 1.0 / sigma
    for turn in range(SWEEPS):
        total = total + direction
        residual = residual - operator * direction
        if turn + 1 < SWEEPS:
            following = 1.0 / (2.0 * sigma - rho)
            direction = following * rho * direction + (2.0 * following / radius) * residual
            rho = following
    return centre, radius, [float(c) for c in total.coef]


def lane_mixers():
    along = np.zeros((LANES, LANES), np.float32)
    across = np.zeros((LANES, LANES), np.float32)
    for lane in range(LANES):
        half, cell = divmod(lane, B)
        for by, weight in ((1, -16.0), (-1, -16.0), (2, 1.0), (-2, 1.0)):
            if 0 <= cell + by < B:
                along[half * B + cell + by, lane] = weight
        across[(1 - half) * B + cell, lane] = -16.0
    return jnp.asarray(np.concatenate([along, along, across, across], axis=0), jnp.bfloat16)


def halves(x):
    high = x.astype(jnp.bfloat16)
    return high, (x - high.astype(jnp.float32)).astype(jnp.bfloat16)


def upper_lanes(rows):
    return lax.broadcasted_iota(jnp.int32, (rows, LANES), 1) >= B


def stencil(ref, a, mixers, centre_weight, scale):
    def read(plane, row):
        return ref[pl.ds(a + 2 + plane, SPAN), PAD + row : PAD + row + HALF, :].reshape(SPAN * HALF, LANES)

    here, below, above = read(0, 0), read(0, -1), read(0, 1)
    side = here + jnp.where(upper_lanes(SPAN * HALF), below, above)
    mixed = jnp.dot(
        jnp.concatenate([*halves(here), *halves(side)], axis=1), mixers, preferred_element_type=jnp.float32
    )
    near = read(-1, 0) + read(1, 0)
    far = (read(-2, 0) + read(2, 0)) + (below + above)
    return here, centre_weight * here + scale * (mixed + (far - 16.0 * near))


def over_spans(body):
    def one(i, carry):
        body(i * SPAN)
        return carry

    lax.fori_loop(0, B // SPAN, one, 0)


def clear_edges(ref):
    deep = ref.shape[0]
    zero = jnp.zeros((PAD, LANES), jnp.float32)

    def one(a, carry):
        ref[a, :PAD, :] = zero
        ref[a, PAD + HALF :, :] = zero
        return carry

    lax.fori_loop(0, deep, one, 0, unroll=4)
    if deep == DEEP:
        for a in (0, 1, DEEP - 2, DEEP - 1):
            ref[a] = jnp.zeros((HIGH, LANES), jnp.float32)


def inner_rows(ref):
    lead = (ref.shape[0] - B) // 2
    return ref.at[pl.ds(lead, B), pl.ds(PAD, HALF), :]


def slab_kernel(place, mix, own, low, high, peer, peer_low, peer_high, previous, potential, out, box):
    slab = place[0]
    core = slab & 1
    rows = pl.ds(PAD, HALF)

    @pl.when(pl.program_id(0) == 0)
    def _():
        clear_edges(box)

    here = own[...]
    box[:, rows, :] = here
    zero = jnp.zeros_like(here)
    below = jnp.where(slab > 1, low[...], zero)
    above = jnp.where(slab < place[1] - 2, high[...], zero)
    edge = jnp.where(core == 0, peer_low[...], peer_high[...])
    held = jnp.logical_or(jnp.logical_and(core == 0, slab > 1), jnp.logical_and(core == 1, slab < place[1] - 2))
    near = peer[...] + jnp.where(held, edge, zero)
    far = below + above
    flat = here.reshape(GROUP * HALF, LANES)
    lower = box[:, PAD - 1 : PAD - 1 + HALF, :].reshape(GROUP * HALF, LANES)
    upper = box[:, PAD + 1 : PAD + 1 + HALF, :].reshape(GROUP * HALF, LANES)
    side = flat + jnp.where(upper_lanes(GROUP * HALF), lower, upper)
    mixed = jnp.dot(
        jnp.concatenate([*halves(flat), *halves(side)], axis=1), mix[...], preferred_element_type=jnp.float32
    )
    mixed = (mixed + (lower + upper)).reshape(GROUP, HALF, LANES)
    kinetic = -3.75 * here - (mixed + (far - 16.0 * near)) / 24.0
    out[...] = 2.0 * here - previous[...] + verlet_factor * (kinetic - potential[...] * here)


def shifted_plane(ref, a, offset, upper, cell):
    lead = (ref.shape[0] - B) // 2
    o0, o1, o2 = offset
    half = lax.shift_right_arithmetic(o1, 1)
    odd = o1 & 1
    source = a + o0
    inside = jnp.logical_and(source >= 0, source < B)
    source = jnp.clip(source, 0, B - 1) + lead
    low = ref[source, pl.ds(PAD + half, HALF), :]
    high = ref[source, pl.ds(PAD + half + odd, HALF), :]
    mixed = jnp.where(upper == (odd == 1), low, high)
    turned = pltpu.roll(mixed, (2 * LANES - o2 - B * odd) & (LANES - 1), 1)
    reached = cell + o2
    keep = jnp.logical_and(jnp.logical_and(reached >= 0, reached < B), inside)
    return jnp.where(keep, turned, 0.0)


def pairs_kernel(scalars, mix, boxes, peers, kept, sent,
                 own, near, rho, work_a, work_b, moved, force, sems, out_sem):
    core = scalars[0]
    dist = [scalars[1 + q] for q in range(3)]
    own_copy = pltpu.make_async_copy(boxes.at[:, 0], own, sems.at[3])
    own_copy.start()
    sources = {1: peers.at[:, core], 2: boxes.at[:, 1], 3: peers.at[:, 1 + core], 4: boxes.at[:, 2]}
    ends = {0: kept.at[:, 0], 1: sent.at[:, 0], 2: kept.at[:, 1], 3: sent.at[:, 1], 4: kept.at[:, 2]}

    def fetch(source, q):
        pltpu.make_async_copy(source, inner_rows(near.at[q]), sems.at[q]).start()

    def deliver(which, sem):
        pltpu.make_async_copy(force.at[which], ends[which], sem).start()

    def fetch_partner(q):
        for far, source in sources.items():
            pl.when(dist[q] == far)(functools.partial(fetch, source, q))

    fetch_partner(0)
    absent = 10 - dist[0] - dist[1] - dist[2]

    def blank(a, carry):
        force[absent, a] = jnp.zeros((HALF, LANES), jnp.float32)
        force[0, a] = jnp.zeros((HALF, LANES), jnp.float32)
        return carry

    lax.fori_loop(0, B, blank, 0, unroll=4)
    for q in range(3):
        clear_edges(near.at[q])
    for buffer in (rho, work_a, work_b):
        clear_edges(buffer)
    cell = lax.broadcasted_iota(jnp.int32, (HALF, LANES), 1) & (B - 1)
    upper = upper_lanes(HALF)
    mixers = mix[...]
    centre, radius, poly = sweep_polynomial()
    poly = [exact_share * c for c in poly]
    centre_weight = (7.5 - centre) / radius
    scale = 1.0 / 12.0 / radius
    rows = pl.ds(PAD, HALF)
    own_copy.wait()
    fetch_partner(1)
    fetch_partner(2)
    for which in sources:
        pl.when(absent == which)(functools.partial(deliver, which, out_sem.at[3]))

    def pair(q, carry):
        offset = tuple(scalars[4 + 3 * q + k] for k in range(3))
        back = tuple(-o for o in offset)
        partner = near.at[q]
        target = scalars[1 + q]
        pltpu.make_async_copy(boxes.at[:, 0], inner_rows(partner), sems.at[q]).wait()

        def overlap(a, carry):
            there = shifted_plane(partner, a, offset, upper, cell)
            moved[a] = there
            rho[a + 2, rows, :] = own[a] * there
            return carry

        def sweep_one(a):
            here, found = stencil(rho, a, mixers, poly[3] * centre_weight, poly[3] * scale)
            work_a[pl.ds(a + 2, SPAN), rows, :] = (found + poly[2] * here).reshape(SPAN, HALF, LANES)

        def sweep_two(a):
            _, found = stencil(work_a, a, mixers, centre_weight, scale)
            found = found.reshape(SPAN, HALF, LANES)
            work_b[pl.ds(a + 2, SPAN), rows, :] = found + poly[1] * rho[pl.ds(a + 2, SPAN), rows, :]

        def sweep_three(a):
            _, found = stencil(work_b, a, mixers, centre_weight, scale)
            here = pl.ds(a, SPAN)
            inner = pl.ds(a + 2, SPAN)
            found = found.reshape(SPAN, HALF, LANES) + poly[0] * rho[inner, rows, :]
            force[0, here] += found * moved[here]
            work_a[inner, rows, :] = found * own[here]

        def give(a, carry):
            force[target, a] = shifted_plane(work_a, a, back, upper, cell)
            return carry

        lax.fori_loop(0, B, overlap, 0, unroll=64)
        over_spans(sweep_one)
        over_spans(sweep_two)
        over_spans(sweep_three)
        pl.when(q == 2)(functools.partial(deliver, 0, out_sem.at[4]))
        lax.fori_loop(0, B, give, 0, unroll=64)
        for which in sources:
            pl.when(target == which)(functools.partial(deliver, which, out_sem.at[q]))
        return carry

    lax.fori_loop(0, 3, pair, 0)
    for k in range(5):
        pltpu.make_async_copy(force.at[0], ends[0], out_sem.at[k]).wait()


F32 = jnp.float32
ANY = pl.BlockSpec(memory_space=pl.ANY)
WHOLE = pl.BlockSpec(memory_space=pltpu.VMEM)
SCALARS = pl.BlockSpec(memory_space=pltpu.SMEM)


def slab_terms(place, arrays):
    block = pl.BlockSpec((GROUP, HALF, LANES), lambda i: (i, 0, 0))
    return pl.pallas_call(
        slab_kernel,
        grid=(arrays[0].shape[0] // GROUP,),
        out_shape=jax.ShapeDtypeStruct(arrays[0].shape, F32),
        in_specs=[SCALARS, WHOLE] + [block] * len(arrays),
        out_specs=block,
        scratch_shapes=[pltpu.VMEM((GROUP, HIGH, LANES), F32)],
        cost_estimate=pl.CostEstimate(flops=20 * B**3, transcendentals=0, bytes_accessed=36 * B**3),
        name="slab",
    )(place, lane_mixers(), *arrays)


def pair_forces(scalars, boxes, peers):
    padded = pltpu.VMEM((DEEP, HIGH, LANES), F32)
    return pl.pallas_call(
        pairs_kernel,
        out_shape=[
            jax.ShapeDtypeStruct((B, 3, HALF, LANES), F32),
            jax.ShapeDtypeStruct((B, 2, HALF, LANES), F32),
        ],
        in_specs=[SCALARS, WHOLE, ANY, ANY],
        out_specs=[ANY, ANY],
        scratch_shapes=[
            pltpu.VMEM((B, HALF, LANES), F32),
            pltpu.VMEM((3, B, HIGH, LANES), F32),
            padded,
            padded,
            padded,
            pltpu.VMEM((B, HALF, LANES), F32),
            pltpu.VMEM((5, B, HALF, LANES), F32),
            pltpu.SemaphoreType.DMA((4,)),
            pltpu.SemaphoreType.DMA((5,)),
        ],
        cost_estimate=pl.CostEstimate(flops=300 * B**3, transcendentals=0, bytes_accessed=40 * B**3),
        name="pairs",
    )(scalars, lane_mixers(), boxes, peers)


def from_behind(array, axis, by):
    count = lax.axis_size(axis)
    return lax.ppermute(array, axis, [(i, (i + by) % count) for i in range(count)])


def core_swap(array):
    count = lax.axis_size("grid")
    return lax.ppermute(array, "grid", [(i, i ^ 1) for i in range(count)])


def local(orbitals, previous, potential, partners, offsets):
    slabs = lax.axis_size("grid")
    total = lax.axis_size("orb") * slabs
    index = lax.axis_index("grid")
    core = index & 1
    place = lax.axis_index(("orb", "grid"))
    dist = jnp.remainder(partners[0] - place, total)
    scalars = jnp.concatenate([core[None], dist, offsets.reshape(-1)])
    slab = jnp.stack([index, jnp.int32(slabs)])

    upper = from_behind(orbitals[:AHEAD], "orb", -1)
    longer = jnp.concatenate([orbitals, upper], axis=0)
    windows = jnp.stack([longer[:slabs], longer[2 : 2 + slabs], longer[4 : 4 + slabs]], axis=1)
    boxes = lax.all_to_all(windows, "grid", split_axis=0, concat_axis=0, tiled=True)
    peers = core_swap(boxes)
    source, _ = lax.optimization_barrier((orbitals, boxes))
    low = from_behind(source, "grid", 2)
    high = from_behind(source, "grid", -2)
    kept, sent = pair_forces(scalars, boxes, peers)
    given = core_swap(sent)
    padded = jnp.pad(given, ((0, 0), (1, 1), (0, 0), (0, 0)))
    summed = kept + lax.dynamic_slice_in_dim(padded, core, 3, axis=1)
    summed, low, high = lax.optimization_barrier((summed, low, high))
    returned = lax.all_to_all(summed, "grid", split_axis=0, concat_axis=0, tiled=True)
    sides = [core_swap(array) for array in (source, low, high)]
    base = slab_terms(slab, [orbitals, low, high, *sides, previous, potential])
    own, two, four = returned[:, 0], returned[:, 1], returned[:, 2]
    spill = four[slabs - 4 :] + jnp.pad(two[slabs - 2 :], ((0, 2), (0, 0), (0, 0)))
    spill = from_behind(spill, "orb", 1)
    exchange_force = own + jnp.concatenate(
        [spill[:2], spill[2:] + two[:2], two[2 : slabs - 2] + four[: slabs - 4]], axis=0
    )
    return base + verlet_factor * exchange_force, exchange_force


def solution(mesh):
    rows = P("orb", "grid", None)
    return jax.shard_map(
        local,
        mesh=mesh,
        in_specs=(rows, rows, rows, P(("orb", "grid"), None), P(("orb", "grid"), None, None)),
        out_specs=(rows, rows),
        check_vma=False,
    )
```

```python
import functools

import jax
import jax.numpy as jnp
import numpy as np
from jax import lax
from jax.experimental import pallas as pl
from jax.experimental.pallas import tpu as pltpu
from jax.sharding import PartitionSpec as P


B = 64
SWEEPS = 4
AHEAD = 4
HALF = B // 2
LANES = 2 * B
PAD = 8
HIGH = HALF + 2 * PAD
DEEP = B + 4
SPAN = 64
GROUP = 8

coulomb_factor = 4.0 * np.pi
exact_share = 0.25
verlet_factor = 0.05
lower_edge = 0.5
upper_edge = 16.0


def sweep_polynomial():
    centre = 0.5 * (upper_edge + lower_edge)
    radius = 0.5 * (upper_edge - lower_edge)
    sigma = centre / radius
    operator = np.polynomial.Polynomial([centre, radius])
    residual = np.polynomial.Polynomial([coulomb_factor])
    direction = residual / centre
    total = np.polynomial.Polynomial([0.0])
    rho = 1.0 / sigma
    for turn in range(SWEEPS):
        total = total + direction
        residual = residual - operator * direction
        if turn + 1 < SWEEPS:
            following = 1.0 / (2.0 * sigma - rho)
            direction = following * rho * direction + (2.0 * following / radius) * residual
            rho = following
    return centre, radius, [float(c) for c in total.coef]


def lane_mixers():
    along = np.zeros((LANES, LANES), np.float32)
    across = np.zeros((LANES, LANES), np.float32)
    for lane in range(LANES):
        half, cell = divmod(lane, B)
        for by, weight in ((1, -16.0), (-1, -16.0), (2, 1.0), (-2, 1.0)):
            if 0 <= cell + by < B:
                along[half * B + cell + by, lane] = weight
        across[(1 - half) * B + cell, lane] = -16.0
    return jnp.asarray(np.concatenate([along, along, across, across], axis=0), jnp.bfloat16)


def halves(x):
    high = x.astype(jnp.bfloat16)
    return high, (x - high.astype(jnp.float32)).astype(jnp.bfloat16)


def upper_lanes(rows):
    return lax.broadcasted_iota(jnp.int32, (rows, LANES), 1) >= B


def stencil(ref, a, mixers, centre_weight, scale):
    def read(plane, row):
        return ref[pl.ds(a + 2 + plane, SPAN), PAD + row : PAD + row + HALF, :].reshape(SPAN * HALF, LANES)

    here, below, above = read(0, 0), read(0, -1), read(0, 1)
    side = here + jnp.where(upper_lanes(SPAN * HALF), below, above)
    mixed = jnp.dot(
        jnp.concatenate([*halves(here), *halves(side)], axis=1), mixers, preferred_element_type=jnp.float32
    )
    near = read(-1, 0) + read(1, 0)
    far = (read(-2, 0) + read(2, 0)) + (below + above)
    return here, centre_weight * here + scale * (mixed + (far - 16.0 * near))


def over_spans(body):
    def one(i, carry):
        body(i * SPAN)
        return carry

    lax.fori_loop(0, B // SPAN, one, 0)


def clear_edges(ref):
    deep = ref.shape[0]
    zero = jnp.zeros((PAD, LANES), jnp.float32)

    def one(a, carry):
        ref[a, :PAD, :] = zero
        ref[a, PAD + HALF :, :] = zero
        return carry

    lax.fori_loop(0, deep, one, 0, unroll=4)
    if deep == DEEP:
        for a in (0, 1, DEEP - 2, DEEP - 1):
            ref[a] = jnp.zeros((HIGH, LANES), jnp.float32)


def inner_rows(ref):
    lead = (ref.shape[0] - B) // 2
    return ref.at[pl.ds(lead, B), pl.ds(PAD, HALF), :]


def slab_kernel(place, mix, own, low, high, peer, peer_low, peer_high, previous, potential, out, box):
    slab = place[0]
    core = slab & 1
    rows = pl.ds(PAD, HALF)

    @pl.when(pl.program_id(0) == 0)
    def _():
        clear_edges(box)

    here = own[...]
    box[:, rows, :] = here
    zero = jnp.zeros_like(here)
    below = jnp.where(slab > 1, low[...], zero)
    above = jnp.where(slab < place[1] - 2, high[...], zero)
    edge = jnp.where(core == 0, peer_low[...], peer_high[...])
    held = jnp.logical_or(jnp.logical_and(core == 0, slab > 1), jnp.logical_and(core == 1, slab < place[1] - 2))
    near = peer[...] + jnp.where(held, edge, zero)
    far = below + above
    flat = here.reshape(GROUP * HALF, LANES)
    lower = box[:, PAD - 1 : PAD - 1 + HALF, :].reshape(GROUP * HALF, LANES)
    upper = box[:, PAD + 1 : PAD + 1 + HALF, :].reshape(GROUP * HALF, LANES)
    side = flat + jnp.where(upper_lanes(GROUP * HALF), lower, upper)
    mixed = jnp.dot(
        jnp.concatenate([*halves(flat), *halves(side)], axis=1), mix[...], preferred_element_type=jnp.float32
    )
    mixed = (mixed + (lower + upper)).reshape(GROUP, HALF, LANES)
    kinetic = -3.75 * here - (mixed + (far - 16.0 * near)) / 24.0
    out[...] = 2.0 * here - previous[...] + verlet_factor * (kinetic - potential[...] * here)


def shifted_plane(ref, a, offset, upper, cell):
    lead = (ref.shape[0] - B) // 2
    o0, o1, o2 = offset
    half = lax.shift_right_arithmetic(o1, 1)
    odd = o1 & 1
    source = a + o0
    inside = jnp.logical_and(source >= 0, source < B)
    source = jnp.clip(source, 0, B - 1) + lead
    low = ref[source, pl.ds(PAD + half, HALF), :]
    high = ref[source, pl.ds(PAD + half + odd, HALF), :]
    mixed = jnp.where(upper == (odd == 1), low, high)
    turned = pltpu.roll(mixed, (2 * LANES - o2 - B * odd) & (LANES - 1), 1)
    reached = cell + o2
    keep = jnp.logical_and(jnp.logical_and(reached >= 0, reached < B), inside)
    return jnp.where(keep, turned, 0.0)


def pairs_kernel(scalars, mix, boxes, peers, kept, sent,
                 own, near, rho, work_a, work_b, moved, force, sems, out_sem):
    core = scalars[0]
    dist = [scalars[1 + q] for q in range(3)]
    own_copy = pltpu.make_async_copy(boxes.at[:, 0], own, sems.at[3])
    own_copy.start()
    sources = {1: peers.at[:, core], 2: boxes.at[:, 1], 3: peers.at[:, 1 + core], 4: boxes.at[:, 2]}
    ends = {0: kept.at[:, 0], 1: sent.at[:, 0], 2: kept.at[:, 1], 3: sent.at[:, 1], 4: kept.at[:, 2]}

    def fetch(source, q):
        pltpu.make_async_copy(source, inner_rows(near.at[q]), sems.at[q]).start()

    def deliver(which, sem):
        pltpu.make_async_copy(force.at[which], ends[which], sem).start()

    def fetch_partner(q):
        for far, source in sources.items():
            pl.when(dist[q] == far)(functools.partial(fetch, source, q))

    fetch_partner(0)
    absent = 10 - dist[0] - dist[1] - dist[2]

    def blank(a, carry):
        force[absent, a] = jnp.zeros((HALF, LANES), jnp.float32)
        force[0, a] = jnp.zeros((HALF, LANES), jnp.float32)
        return carry

    lax.fori_loop(0, B, blank, 0, unroll=4)
    for q in range(3):
        clear_edges(near.at[q])
    for buffer in (rho, work_a, work_b):
        clear_edges(buffer)
    cell = lax.broadcasted_iota(jnp.int32, (HALF, LANES), 1) & (B - 1)
    upper = upper_lanes(HALF)
    mixers = mix[...]
    centre, radius, poly = sweep_polynomial()
    poly = [exact_share * c for c in poly]
    centre_weight = (7.5 - centre) / radius
    scale = 1.0 / 12.0 / radius
    rows = pl.ds(PAD, HALF)
    own_copy.wait()
    fetch_partner(1)
    fetch_partner(2)
    for which in sources:
        pl.when(absent == which)(functools.partial(deliver, which, out_sem.at[3]))

    def pair(q, carry):
        offset = tuple(scalars[4 + 3 * q + k] for k in range(3))
        back = tuple(-o for o in offset)
        partner = near.at[q]
        target = scalars[1 + q]
        pltpu.make_async_copy(boxes.at[:, 0], inner_rows(partner), sems.at[q]).wait()

        def overlap(a, carry):
            there = shifted_plane(partner, a, offset, upper, cell)
            moved[a] = there
            rho[a + 2, rows, :] = own[a] * there
            return carry

        def sweep_one(a):
            here, found = stencil(rho, a, mixers, poly[3] * centre_weight, poly[3] * scale)
            work_a[pl.ds(a + 2, SPAN), rows, :] = (found + poly[2] * here).reshape(SPAN, HALF, LANES)

        def sweep_two(a):
            _, found = stencil(work_a, a, mixers, centre_weight, scale)
            found = found.reshape(SPAN, HALF, LANES)
            work_b[pl.ds(a + 2, SPAN), rows, :] = found + poly[1] * rho[pl.ds(a + 2, SPAN), rows, :]

        def sweep_three(a):
            _, found = stencil(work_b, a, mixers, centre_weight, scale)
            here = pl.ds(a, SPAN)
            inner = pl.ds(a + 2, SPAN)
            found = found.reshape(SPAN, HALF, LANES) + poly[0] * rho[inner, rows, :]
            force[0, here] += found * moved[here]
            work_a[inner, rows, :] = found * own[here]

        def give(a, carry):
            force[target, a] = shifted_plane(work_a, a, back, upper, cell)
            return carry

        lax.fori_loop(0, B, overlap, 0, unroll=64)
        over_spans(sweep_one)
        over_spans(sweep_two)
        over_spans(sweep_three)
        pl.when(q == 2)(functools.partial(deliver, 0, out_sem.at[4]))
        lax.fori_loop(0, B, give, 0, unroll=64)
        for which in sources:
            pl.when(target == which)(functools.partial(deliver, which, out_sem.at[q]))
        return carry

    lax.fori_loop(0, 3, pair, 0)
    for k in range(5):
        pltpu.make_async_copy(force.at[0], ends[0], out_sem.at[k]).wait()


F32 = jnp.float32
ANY = pl.BlockSpec(memory_space=pl.ANY)
WHOLE = pl.BlockSpec(memory_space=pltpu.VMEM)
SCALARS = pl.BlockSpec(memory_space=pltpu.SMEM)


def slab_terms(place, arrays):
    block = pl.BlockSpec((GROUP, HALF, LANES), lambda i: (i, 0, 0))
    return pl.pallas_call(
        slab_kernel,
        grid=(arrays[0].shape[0] // GROUP,),
        out_shape=jax.ShapeDtypeStruct(arrays[0].shape, F32),
        in_specs=[SCALARS, WHOLE] + [block] * len(arrays),
        out_specs=block,
        scratch_shapes=[pltpu.VMEM((GROUP, HIGH, LANES), F32)],
        cost_estimate=pl.CostEstimate(flops=20 * B**3, transcendentals=0, bytes_accessed=36 * B**3),
        name="slab",
    )(place, lane_mixers(), *arrays)


def pair_forces(scalars, boxes, peers):
    padded = pltpu.VMEM((DEEP, HIGH, LANES), F32)
    return pl.pallas_call(
        pairs_kernel,
        out_shape=[
            jax.ShapeDtypeStruct((B, 3, HALF, LANES), F32),
            jax.ShapeDtypeStruct((B, 2, HALF, LANES), F32),
        ],
        in_specs=[SCALARS, WHOLE, ANY, ANY],
        out_specs=[ANY, ANY],
        scratch_shapes=[
            pltpu.VMEM((B, HALF, LANES), F32),
            pltpu.VMEM((3, B, HIGH, LANES), F32),
            padded,
            padded,
            padded,
            pltpu.VMEM((B, HALF, LANES), F32),
            pltpu.VMEM((5, B, HALF, LANES), F32),
            pltpu.SemaphoreType.DMA((4,)),
            pltpu.SemaphoreType.DMA((5,)),
        ],
        cost_estimate=pl.CostEstimate(flops=300 * B**3, transcendentals=0, bytes_accessed=40 * B**3),
        name="pairs",
    )(scalars, lane_mixers(), boxes, peers)


def from_behind(array, axis, by):
    count = lax.axis_size(axis)
    return lax.ppermute(array, axis, [(i, (i + by) % count) for i in range(count)])


def core_swap(array):
    count = lax.axis_size("grid")
    return lax.ppermute(array, "grid", [(i, i ^ 1) for i in range(count)])


def local(orbitals, previous, potential, partners, offsets):
    slabs = lax.axis_size("grid")
    total = lax.axis_size("orb") * slabs
    index = lax.axis_index("grid")
    core = index & 1
    place = lax.axis_index(("orb", "grid"))
    dist = jnp.remainder(partners[0] - place, total)
    scalars = jnp.concatenate([core[None], dist, offsets.reshape(-1)])
    slab = jnp.stack([index, jnp.int32(slabs)])

    upper = from_behind(orbitals[:AHEAD], "orb", -1)
    longer = jnp.concatenate([orbitals, upper], axis=0)
    windows = jnp.stack([longer[:slabs], longer[2 : 2 + slabs], longer[4 : 4 + slabs]], axis=1)
    windows, scalars = lax.optimization_barrier((windows, scalars))
    boxes = lax.all_to_all(windows, "grid", split_axis=0, concat_axis=0, tiled=True)
    peers = core_swap(boxes)
    source, _ = lax.optimization_barrier((orbitals, boxes))
    low = from_behind(source, "grid", 2)
    high = from_behind(source, "grid", -2)
    kept, sent = pair_forces(scalars, boxes, peers)
    given = core_swap(sent)
    summed = lax.dynamic_update_slice_in_dim(
        kept, lax.dynamic_slice_in_dim(kept, 1 - core, 2, axis=1) + given, 1 - core, axis=1
    )
    returned = lax.all_to_all(summed, "grid", split_axis=0, concat_axis=0, tiled=True)
    sides = [core_swap(array) for array in (source, low, high)]
    base = slab_terms(slab, [orbitals, low, high, *sides, previous, potential])
    own, two, four = returned[:, 0], returned[:, 1], returned[:, 2]
    spill = four[slabs - 4 :] + jnp.pad(two[slabs - 2 :], ((0, 2), (0, 0), (0, 0)))
    spill = from_behind(spill, "orb", 1)
    exchange_force = own + jnp.concatenate(
        [spill[:2], spill[2:] + two[:2], two[2 : slabs - 2] + four[: slabs - 4]], axis=0
    )
    return base + verlet_factor * exchange_force, exchange_force


def solution(mesh):
    rows = P("orb", "grid", None)
    return jax.shard_map(
        local,
        mesh=mesh,
        in_specs=(rows, rows, rows, P(("orb", "grid"), None), P(("orb", "grid"), None, None)),
        out_specs=(rows, rows),
        check_vma=False,
    )
```

```python
import functools

import jax
import jax.numpy as jnp
import numpy as np
from jax import lax
from jax.experimental import pallas as pl
from jax.experimental.pallas import tpu as pltpu
from jax.sharding import PartitionSpec as P


B = 64
SWEEPS = 4
AHEAD = 4
HALF = B // 2
LANES = 2 * B
PAD = 8
HIGH = HALF + 2 * PAD
DEEP = B + 4
SPAN = 64
GROUP = 8

coulomb_factor = 4.0 * np.pi
exact_share = 0.25
verlet_factor = 0.05
lower_edge = 0.5
upper_edge = 16.0


def sweep_polynomial():
    centre = 0.5 * (upper_edge + lower_edge)
    radius = 0.5 * (upper_edge - lower_edge)
    sigma = centre / radius
    operator = np.polynomial.Polynomial([centre, radius])
    residual = np.polynomial.Polynomial([coulomb_factor])
    direction = residual / centre
    total = np.polynomial.Polynomial([0.0])
    rho = 1.0 / sigma
    for turn in range(SWEEPS):
        total = total + direction
        residual = residual - operator * direction
        if turn + 1 < SWEEPS:
            following = 1.0 / (2.0 * sigma - rho)
            direction = following * rho * direction + (2.0 * following / radius) * residual
            rho = following
    return centre, radius, [float(c) for c in total.coef]


def lane_mixers():
    along = np.zeros((LANES, LANES), np.float32)
    across = np.zeros((LANES, LANES), np.float32)
    for lane in range(LANES):
        half, cell = divmod(lane, B)
        for by, weight in ((1, -16.0), (-1, -16.0), (2, 1.0), (-2, 1.0)):
            if 0 <= cell + by < B:
                along[half * B + cell + by, lane] = weight
        across[(1 - half) * B + cell, lane] = -16.0
    return jnp.asarray(np.concatenate([along, along, across, across], axis=0), jnp.bfloat16)


def halves(x):
    high = x.astype(jnp.bfloat16)
    return high, (x - high.astype(jnp.float32)).astype(jnp.bfloat16)


def upper_lanes(rows):
    return lax.broadcasted_iota(jnp.int32, (rows, LANES), 1) >= B


def stencil(ref, a, mixers, centre_weight, scale):
    def read(plane, row):
        return ref[pl.ds(a + 2 + plane, SPAN), PAD + row : PAD + row + HALF, :].reshape(SPAN * HALF, LANES)

    here, below, above = read(0, 0), read(0, -1), read(0, 1)
    side = here + jnp.where(upper_lanes(SPAN * HALF), below, above)
    mixed = jnp.dot(
        jnp.concatenate([*halves(here), *halves(side)], axis=1), mixers, preferred_element_type=jnp.float32
    )
    near = read(-1, 0) + read(1, 0)
    far = (read(-2, 0) + read(2, 0)) + (below + above)
    return here, centre_weight * here + scale * (mixed + (far - 16.0 * near))


def over_spans(body):
    def one(i, carry):
        body(i * SPAN)
        return carry

    lax.fori_loop(0, B // SPAN, one, 0)


def clear_edges(ref):
    deep = ref.shape[0]
    zero = jnp.zeros((PAD, LANES), jnp.float32)

    def one(a, carry):
        ref[a, :PAD, :] = zero
        ref[a, PAD + HALF :, :] = zero
        return carry

    lax.fori_loop(0, deep, one, 0, unroll=4)
    if deep == DEEP:
        for a in (0, 1, DEEP - 2, DEEP - 1):
            ref[a] = jnp.zeros((HIGH, LANES), jnp.float32)


def inner_rows(ref):
    lead = (ref.shape[0] - B) // 2
    return ref.at[pl.ds(lead, B), pl.ds(PAD, HALF), :]


def slab_kernel(place, mix, own, low, high, peer, peer_low, peer_high, previous, potential, out, box):
    slab = place[0]
    core = slab & 1
    rows = pl.ds(PAD, HALF)

    @pl.when(pl.program_id(0) == 0)
    def _():
        clear_edges(box)

    here = own[...]
    box[:, rows, :] = here
    zero = jnp.zeros_like(here)
    below = jnp.where(slab > 1, low[...], zero)
    above = jnp.where(slab < place[1] - 2, high[...], zero)
    edge = jnp.where(core == 0, peer_low[...], peer_high[...])
    held = jnp.logical_or(jnp.logical_and(core == 0, slab > 1), jnp.logical_and(core == 1, slab < place[1] - 2))
    near = peer[...] + jnp.where(held, edge, zero)
    far = below + above
    flat = here.reshape(GROUP * HALF, LANES)
    lower = box[:, PAD - 1 : PAD - 1 + HALF, :].reshape(GROUP * HALF, LANES)
    upper = box[:, PAD + 1 : PAD + 1 + HALF, :].reshape(GROUP * HALF, LANES)
    side = flat + jnp.where(upper_lanes(GROUP * HALF), lower, upper)
    mixed = jnp.dot(
        jnp.concatenate([*halves(flat), *halves(side)], axis=1), mix[...], preferred_element_type=jnp.float32
    )
    mixed = (mixed + (lower + upper)).reshape(GROUP, HALF, LANES)
    kinetic = -3.75 * here - (mixed + (far - 16.0 * near)) / 24.0
    out[...] = 2.0 * here - previous[...] + verlet_factor * (kinetic - potential[...] * here)


def shifted_plane(ref, a, offset, upper, cell):
    lead = (ref.shape[0] - B) // 2
    o0, o1, o2 = offset
    half = lax.shift_right_arithmetic(o1, 1)
    odd = o1 & 1
    source = a + o0
    inside = jnp.logical_and(source >= 0, source < B)
    source = jnp.clip(source, 0, B - 1) + lead
    low = ref[source, pl.ds(PAD + half, HALF), :]
    high = ref[source, pl.ds(PAD + half + odd, HALF), :]
    mixed = jnp.where(upper == (odd == 1), low, high)
    turned = pltpu.roll(mixed, (2 * LANES - o2 - B * odd) & (LANES - 1), 1)
    reached = cell + o2
    keep = jnp.logical_and(jnp.logical_and(reached >= 0, reached < B), inside)
    return jnp.where(keep, turned, 0.0)


def pairs_kernel(partners, offsets, mix, boxes, peers, kept, sent,
                 own, near, rho, work_a, work_b, moved, force, sems, out_sem):
    core = lax.axis_index("grid") & 1
    total = lax.axis_size("orb") * lax.axis_size("grid")
    place = lax.axis_index("orb") * lax.axis_size("grid") + lax.axis_index("grid")
    dist = [lax.rem(partners[0, q] - place + total, total) for q in range(3)]
    own_copy = pltpu.make_async_copy(boxes.at[:, 0], own, sems.at[3])
    own_copy.start()
    sources = {1: peers.at[:, core], 2: boxes.at[:, 1], 3: peers.at[:, 1 + core], 4: boxes.at[:, 2]}
    ends = {0: kept.at[:, 0], 1: sent.at[:, 0], 2: kept.at[:, 1], 3: sent.at[:, 1], 4: kept.at[:, 2]}

    def fetch(source, q):
        pltpu.make_async_copy(source, inner_rows(near.at[q]), sems.at[q]).start()

    def deliver(which, sem):
        pltpu.make_async_copy(force.at[which], ends[which], sem).start()

    def fetch_partner(q):
        for far, source in sources.items():
            pl.when(dist[q] == far)(functools.partial(fetch, source, q))

    fetch_partner(0)
    absent = 10 - dist[0] - dist[1] - dist[2]

    def blank(a, carry):
        force[absent, a] = jnp.zeros((HALF, LANES), jnp.float32)
        force[0, a] = jnp.zeros((HALF, LANES), jnp.float32)
        return carry

    lax.fori_loop(0, B, blank, 0, unroll=4)
    for q in range(3):
        clear_edges(near.at[q])
    for buffer in (rho, work_a, work_b):
        clear_edges(buffer)
    cell = lax.broadcasted_iota(jnp.int32, (HALF, LANES), 1) & (B - 1)
    upper = upper_lanes(HALF)
    mixers = mix[...]
    centre, radius, poly = sweep_polynomial()
    poly = [exact_share * c for c in poly]
    centre_weight = (7.5 - centre) / radius
    scale = 1.0 / 12.0 / radius
    rows = pl.ds(PAD, HALF)
    own_copy.wait()
    fetch_partner(1)
    fetch_partner(2)
    for which in sources:
        pl.when(absent == which)(functools.partial(deliver, which, out_sem.at[3]))

    def pair(q, carry):
        offset = tuple(offsets[0, q, k] for k in range(3))
        back = tuple(-o for o in offset)
        partner = near.at[q]
        target = jnp.where(q == 0, dist[0], jnp.where(q == 1, dist[1], dist[2]))
        pltpu.make_async_copy(boxes.at[:, 0], inner_rows(partner), sems.at[q]).wait()

        def overlap(a, carry):
            there = shifted_plane(partner, a, offset, upper, cell)
            moved[a] = there
            rho[a + 2, rows, :] = own[a] * there
            return carry

        def sweep_one(a):
            here, found = stencil(rho, a, mixers, poly[3] * centre_weight, poly[3] * scale)
            work_a[pl.ds(a + 2, SPAN), rows, :] = (found + poly[2] * here).reshape(SPAN, HALF, LANES)

        def sweep_two(a):
            _, found = stencil(work_a, a, mixers, centre_weight, scale)
            found = found.reshape(SPAN, HALF, LANES)
            work_b[pl.ds(a + 2, SPAN), rows, :] = found + poly[1] * rho[pl.ds(a + 2, SPAN), rows, :]

        def sweep_three(a):
            _, found = stencil(work_b, a, mixers, centre_weight, scale)
            here = pl.ds(a, SPAN)
            inner = pl.ds(a + 2, SPAN)
            found = found.reshape(SPAN, HALF, LANES) + poly[0] * rho[inner, rows, :]
            force[0, here] += found * moved[here]
            work_a[inner, rows, :] = found * own[here]

        def give(a, carry):
            force[target, a] = shifted_plane(work_a, a, back, upper, cell)
            return carry

        lax.fori_loop(0, B, overlap, 0, unroll=64)
        over_spans(sweep_one)
        over_spans(sweep_two)
        over_spans(sweep_three)
        pl.when(q == 2)(functools.partial(deliver, 0, out_sem.at[4]))
        lax.fori_loop(0, B, give, 0, unroll=64)
        for which in sources:
            pl.when(target == which)(functools.partial(deliver, which, out_sem.at[q]))
        return carry

    lax.fori_loop(0, 3, pair, 0)
    for k in range(5):
        pltpu.make_async_copy(force.at[0], ends[0], out_sem.at[k]).wait()


F32 = jnp.float32
ANY = pl.BlockSpec(memory_space=pl.ANY)
WHOLE = pl.BlockSpec(memory_space=pltpu.VMEM)
SCALARS = pl.BlockSpec(memory_space=pltpu.SMEM)


def slab_terms(place, arrays):
    block = pl.BlockSpec((GROUP, HALF, LANES), lambda i: (i, 0, 0))
    return pl.pallas_call(
        slab_kernel,
        grid=(arrays[0].shape[0] // GROUP,),
        out_shape=jax.ShapeDtypeStruct(arrays[0].shape, F32),
        in_specs=[SCALARS, WHOLE] + [block] * len(arrays),
        out_specs=block,
        scratch_shapes=[pltpu.VMEM((GROUP, HIGH, LANES), F32)],
        cost_estimate=pl.CostEstimate(flops=20 * B**3, transcendentals=0, bytes_accessed=36 * B**3),
        name="slab",
    )(place, lane_mixers(), *arrays)


def pair_forces(partners, offsets, boxes, peers):
    padded = pltpu.VMEM((DEEP, HIGH, LANES), F32)
    return pl.pallas_call(
        pairs_kernel,
        out_shape=[
            jax.ShapeDtypeStruct((B, 3, HALF, LANES), F32),
            jax.ShapeDtypeStruct((B, 2, HALF, LANES), F32),
        ],
        in_specs=[SCALARS, SCALARS, WHOLE, ANY, ANY],
        out_specs=[ANY, ANY],
        scratch_shapes=[
            pltpu.VMEM((B, HALF, LANES), F32),
            pltpu.VMEM((3, B, HIGH, LANES), F32),
            padded,
            padded,
            padded,
            pltpu.VMEM((B, HALF, LANES), F32),
            pltpu.VMEM((5, B, HALF, LANES), F32),
            pltpu.SemaphoreType.DMA((4,)),
            pltpu.SemaphoreType.DMA((5,)),
        ],
        cost_estimate=pl.CostEstimate(flops=300 * B**3, transcendentals=0, bytes_accessed=40 * B**3),
        name="pairs",
    )(partners, offsets, lane_mixers(), boxes, peers)


def from_behind(array, axis, by):
    count = lax.axis_size(axis)
    return lax.ppermute(array, axis, [(i, (i + by) % count) for i in range(count)])


def core_swap(array):
    count = lax.axis_size("grid")
    return lax.ppermute(array, "grid", [(i, i ^ 1) for i in range(count)])


def local(orbitals, previous, potential, partners, offsets):
    slabs = lax.axis_size("grid")
    index = lax.axis_index("grid")
    core = index & 1
    slab = jnp.stack([index, jnp.int32(slabs)])

    upper = from_behind(orbitals[:AHEAD], "orb", -1)
    longer = jnp.concatenate([orbitals, upper], axis=0)
    windows = jnp.stack([longer[:slabs], longer[2 : 2 + slabs], longer[4 : 4 + slabs]], axis=1)
    boxes = lax.all_to_all(windows, "grid", split_axis=0, concat_axis=0, tiled=True)
    peers = core_swap(boxes)
    source, _ = lax.optimization_barrier((orbitals, boxes))
    low = from_behind(source, "grid", 2)
    high = from_behind(source, "grid", -2)
    kept, sent = pair_forces(partners, offsets, boxes, peers)
    given = core_swap(sent)
    summed = lax.dynamic_update_slice_in_dim(
        kept, lax.dynamic_slice_in_dim(kept, 1 - core, 2, axis=1) + given, 1 - core, axis=1
    )
    returned = lax.all_to_all(summed, "grid", split_axis=0, concat_axis=0, tiled=True)
    sides = [core_swap(array) for array in (source, low, high)]
    base = slab_terms(slab, [orbitals, low, high, *sides, previous, potential])
    own, two, four = returned[:, 0], returned[:, 1], returned[:, 2]
    spill = four[slabs - 4 :] + jnp.pad(two[slabs - 2 :], ((0, 2), (0, 0), (0, 0)))
    spill = from_behind(spill, "orb", 1)
    exchange_force = own + jnp.concatenate(
        [spill[:2], spill[2:] + two[:2], two[2 : slabs - 2] + four[: slabs - 4]], axis=0
    )
    return base + verlet_factor * exchange_force, exchange_force


def solution(mesh):
    rows = P("orb", "grid", None)
    return jax.shard_map(
        local,
        mesh=mesh,
        in_specs=(rows, rows, rows, P(("orb", "grid"), None), P(("orb", "grid"), None, None)),
        out_specs=(rows, rows),
        check_vma=False,
    )
```
